32 devices in a mesh: occ: 8 (over y, x, core), frag: 4 (over z).
Axes of the slice: x: 2, y: 2, z: 4, core: 2. Of those that a mesh axis runs over, the one named last changes fastest.
Arguments:
- factors: bfloat16 [32, 512, 1280], P(('frag', 'occ')), parts along dimension 0, may hold values from -1 to 1
- occ_energy: float32 [32], P('frag'), parts along dimension 0, may hold values from -2 to -0.3
- vir_energy: float32 [2048], P('frag'), parts along dimension 0, may hold values from 0.2 to 4
- coeffs: bfloat16 [4096, 512], P('frag'), parts along dimension 0, may hold values from -0.25 to 0.25
Outputs:
- back: bfloat16 [1280, 32, 1024], P('occ', 'frag'), parts along dimension 1
The draws below stay inside these ranges and needn't reach their ends.
There are 4 independent parts, one for each index of `frag`. The reference program is written for one: setup_inputs(seed, part) draws one part's arguments, and reference() takes and returns one part's arrays. A program takes and returns all parts, laid end to end along the dimension named above; each array names one. Nothing has to cross between parts.
All inputs are finite; a program needn't handle non-finite values.
Results may differ from the reference program's by a relative error of at most 0.008.
Values may be sent and summed in bfloat16 or wider, within the bound.
A program may use at most 64 MiB of HBM per device.

```python
import jax
import jax.numpy as jnp
from jax import lax

V = 512
A = 1280
NAO = 1024
OFFSETS = 3
OCC = 8


def steps_of(own_key, extent, cuts, least, high):
    def one(position, shards_of):
        steps = jax.random.uniform(jax.random.fold_in(jax.random.fold_in(own_key, 6), position), (shards_of,), jnp.float32, least / len(cuts), high / len(cuts))
        return jnp.repeat(jnp.exp(steps), extent[position] // shards_of).reshape((-1,) + (1,) * (len(extent) - position - 1))

    loudness = one(*cuts[0])
    for cut in cuts[1:]:
        loudness = loudness * one(*cut)
    return loudness


def normal_values(own_key, extent, scale, bound, shards=(), held_as=jnp.bfloat16):
    gain = steps_of(own_key, extent, shards, -0.22, 0.18) if shards else 1.0
    array = jax.random.normal(own_key, extent, jnp.float32) * scale * gain
    return jnp.minimum(jnp.maximum(array, -bound), bound).astype(held_as)


def setup_inputs(seed: int = 0, part: int = 0) -> dict:
    seeds = jax.random.split(jax.random.key(seed), 5)
    own_keys = jax.random.split(jax.random.fold_in(seeds[4], part), 5)
    return {
        "factors": normal_values(own_keys[0], (OCC, V, A), 0.17, 1.0, ((0, 8),)),
        "occ_energy": jnp.clip(jax.random.uniform(own_keys[1], (OCC,), jnp.float32, -2.0, -0.3), -2.0, -0.3),
        "vir_energy": jnp.clip(jax.random.uniform(own_keys[2], (V,), jnp.float32, 0.2, 4.0), 0.2, 4.0),
        "coeffs": normal_values(own_keys[3], (NAO, V), V ** -0.5, 0.25),
    }


def rounded(value):
    return lax.optimization_barrier(value.astype(jnp.bfloat16)).astype(jnp.float32)


def reference(factors, occ_energy, vir_energy, coeffs):
    mine = factors.astype(jnp.float32)
    own = jnp.zeros((OCC, A, V), jnp.float32)
    incoming = jnp.zeros((OCC, A, V), jnp.float32)
    for offset in range(1, OFFSETS + 1):
        partner = jnp.roll(mine, -offset, axis=0)
        pair_energy = occ_energy + jnp.roll(occ_energy, -offset)
        kmat = jnp.einsum('iap,ibp->iab', mine, partner)
        denom = pair_energy[:, None, None] - vir_energy[None, :, None] - vir_energy[None, None, :]
        amps = rounded(kmat / denom)
        own = own + jnp.einsum('iab,ibp->ipa', amps, partner)
        sent = rounded(jnp.einsum('iap,iab->ipb', mine, amps))
        incoming = incoming + jnp.roll(sent, offset, axis=0)
    gamma = rounded(own + incoming)
    return jnp.einsum('ipa,ma->pim', gamma, coeffs.astype(jnp.float32)).astype(jnp.bfloat16)
```

```python
import jax
import jax.numpy as jnp
from jax import lax
from jax.experimental import pallas as pl
from jax.experimental.pallas import tpu as pltpu
from jax.sharding import PartitionSpec as P

OFFSETS = 3


def passed_along(block, axis, distance):
    devices = range(lax.axis_size(axis))
    route = [((i - distance) % len(devices), i) for i in devices]
    return lax.ppermute(block, axis, route)


def on_device(factors, occ_energy, vir_energy, coeffs):
    mine = factors[0]
    count = lax.axis_size("occ")
    index = lax.axis_index("occ")
    partners = []
    current = mine
    for offset in range(1, OFFSETS + 1):
        current = passed_along(current, "occ", -1)
        partners.append(current)
    own_energy = lax.dynamic_index_in_dim(occ_energy, index, 0, False)
    own = jnp.zeros((mine.shape[1], mine.shape[0]), jnp.float32)
    outgoing = []
    for offset in range(1, OFFSETS + 1):
        partner = partners[offset - 1]
        other_energy = lax.dynamic_index_in_dim(occ_energy, (index + offset) % count, 0, False)
        kmat = lax.dot_general(
            mine, partner, (((1,), (1,)), ((), ())), preferred_element_type=jnp.float32
        )
        denom = own_energy + other_energy - vir_energy[:, None] - vir_energy[None, :]
        amps = (kmat / denom).astype(jnp.bfloat16)
        own = own + lax.dot_general(
            partner, amps, (((0,), (1,)), ((), ())), preferred_element_type=jnp.float32
        )
        sent = lax.dot_general(
            mine, amps, (((0,), (0,)), ((), ())), preferred_element_type=jnp.float32
        )
        outgoing.append(sent.astype(jnp.bfloat16))
    incoming = jnp.zeros_like(own)
    for offset in range(1, OFFSETS + 1):
        arrived = passed_along(outgoing[offset - 1], "occ", offset)
        incoming = incoming + arrived.astype(jnp.float32)
    gamma = (own + incoming).astype(jnp.bfloat16)[None]
    slabs = lax.all_to_all(gamma, "occ", split_axis=1, concat_axis=0, tiled=True)
    return jnp.einsum("ipa,ma->pim", slabs, coeffs, preferred_element_type=jnp.float32).astype(
        jnp.bfloat16
    )


LANES = 128
ROWS = 128
CHUNK = ROWS // 2

NEAR_U = (2, 2, 3, 3, 4, 5)
NEAR_V = (0, 1, 0, 1, 1, 0)
SIDE_U = (2, 2, 2, 3, 3, 4)
SIDE_V = (3, 4, 5, 4, 5, 5)
FAR_U = (6, 6, 6, 6, 6, 7, 7, 7, 7, 7)
FAR_V = (0, 1, 3, 4, 5, 0, 1, 2, 4, 5)


def flipped(a, b):
    bits = [(a // w % 2 + b // w % 2) % 2 * w for w in (1, 2, 4)]
    return bits[0] + bits[1] + bits[2]


def entry(table, n):
    packed = sum(value << (3 * k) for k, value in enumerate(table))
    return lax.shift_right_logical(jnp.int32(packed), jnp.int32(3) * n) % 8


def gathered_kernel(
    mine_ref, energy_ref, vir_ref, out_ref,
    blocks, slabs, total, turned, vcol, local_sem, own_sem, fwd_sem, sib_sem, recv_sem,
):
    me = lax.axis_index("occ")
    virtuals, depth = mine_ref.shape
    width = total.shape[1]
    window = turned.shape[0]
    steps = virtuals // ROWS
    chunks = virtuals // CHUNK
    first = me * width
    lead = pl.multiple_of(first // LANES * LANES, LANES)
    skip = pl.multiple_of(first % LANES, 32)

    barrier = pltpu.get_barrier_semaphore()
    for bit in (1, 2, 4):
        pl.semaphore_signal(
            barrier, inc=1, device_id={"occ": flipped(me, bit)},
            device_id_type=pl.DeviceIdType.MESH,
        )
    pl.semaphore_wait(barrier, 3)

    def rows_of(q):
        return pl.ds(pl.multiple_of(q * CHUNK, CHUNK), CHUNK)

    def send(source, label, q, bit, send_sem):
        return pltpu.make_async_remote_copy(
            src_ref=source,
            dst_ref=blocks.at[flipped(me, label), rows_of(q)],
            send_sem=send_sem,
            recv_sem=recv_sem.at[flipped(label, bit), q],
            device_id={"occ": flipped(me, bit)},
            device_id_type=pl.DeviceIdType.MESH,
        )

    def own_send(q, axis):
        return send(mine_ref.at[rows_of(q)], 0, q, 2 + 2 * axis, own_sem.at[axis, q])

    def far_send(q, label):
        return send(
            blocks.at[flipped(me, label), rows_of(q)], label, q, 6 - label, fwd_sem.at[q]
        )

    def sib_send(q, label):
        source = mine_ref.at[rows_of(q)] if label == 0 else blocks.at[flipped(me, label), rows_of(q)]
        return send(source, label, q, 1, sib_sem.at[label // 2, q])

    def arrived(label, q):
        place = blocks.at[flipped(me, label), rows_of(q)]
        pltpu.make_async_copy(place, place, recv_sem.at[label, q]).wait()

    @pl.loop(0, chunks)
    def _(q):
        own_send(q, 0).start()
        own_send(q, 1).start()
        sib_send(q, 0).start()

    local = pltpu.make_async_copy(mine_ref, blocks.at[me], local_sem)
    local.start()
    total[...] = jnp.zeros_like(total)
    for t in range(steps):
        part = vir_ref[:, t * ROWS:(t + 1) * ROWS]
        vcol[t * ROWS:(t + 1) * ROWS, :] = jnp.broadcast_to(part, (ROWS, ROWS)).T
    local.wait()

    def turn(label, t):
        u = flipped(me, label)
        rows = pl.ds(pl.multiple_of(t * ROWS, ROWS), ROWS)
        turned[...] = blocks[u, rows, pl.ds(lead, window)].astype(jnp.float32).T
        slabs[u, :, rows] = turned[pl.ds(skip, width), :].astype(jnp.bfloat16)

    def pair(label_u, label_v, t):
        u, v = flipped(me, label_u), flipped(me, label_v)
        rows = pl.ds(pl.multiple_of(t * ROWS, ROWS), ROWS)
        kmat = lax.dot_general(
            blocks[u, rows, :], blocks[v], (((1,), (1,)), ((), ())),
            preferred_element_type=jnp.float32,
        )
        denom = energy_ref[u] + energy_ref[v] - vcol[rows, 0:1] - vir_ref[...]
        amps = (kmat / denom).astype(jnp.bfloat16)
        total[v] += jnp.dot(slabs[u, :, rows], amps, preferred_element_type=jnp.float32)
        total[u, :, rows] += lax.dot_general(
            slabs[v], amps, (((1,), (1,)), ((), ())), preferred_element_type=jnp.float32
        )

    @pl.loop(0, chunks)
    def _(q):
        arrived(1, q)

    @pl.loop(0, steps)
    def _(t):
        turn(0, t)
        turn(1, t)

    @pl.loop(0, steps)
    def _(t):
        pair(0, 1, t)

    @pl.loop(0, steps)
    def _(t):
        for k in (0, 1):
            q = 2 * t + k
            arrived(2, q)
            sib_send(q, 2).start()
            if k == 0:
                far_send(q, 2).start()
            arrived(4, q)
            sib_send(q, 4).start()
            if k == 1:
                far_send(q, 4).start()
        turn(2, t)
        turn(4, t)
        for k in (0, 1):
            arrived(3, 2 * t + k)
            arrived(5, 2 * t + k)
        turn(3, t)
        turn(5, t)

        @pl.loop(0, len(NEAR_U))
        def _(n):
            pair(entry(NEAR_U, n), entry(NEAR_V, n), t)

    @pl.loop(0, steps)
    def _(t):
        @pl.loop(0, len(SIDE_U))
        def _(n):
            pair(entry(SIDE_U, n), entry(SIDE_V, n), t)

        for k in (0, 1):
            q = 2 * t + k
            arrived(6, q)
            sib_send(q, 6).start()
        turn(6, t)
        for k in (0, 1):
            arrived(7, 2 * t + k)
        turn(7, t)

        @pl.loop(0, len(FAR_U))
        def _(n):
            pair(entry(FAR_U, n), entry(FAR_V, n), t)

    @pl.loop(0, steps)
    def _(t):
        pair(6, 7, t)

    @pl.loop(0, 2 * OFFSETS + 2)
    def _(u):
        out_ref[u] = total[u].astype(jnp.bfloat16)

    @pl.loop(0, steps)
    def _(t):
        for k in (0, 1):
            q = 2 * t + k
            own_send(q, 0).wait_send()
            own_send(q, 1).wait_send()
            for label in (0, 2, 4, 6):
                sib_send(q, label).wait_send()
            far_send(q, 2 if k == 0 else 4).wait_send()


def gathered(factors, occ_energy, vir_energy, coeffs):
    _, virtuals, depth = factors.shape
    count = lax.axis_size("occ")
    width = depth // count
    window = max(
        -(-(d * width % LANES + width) // LANES) * LANES for d in range(count)
    )
    steps = virtuals // ROWS
    chunks = virtuals // CHUNK
    pair_flops = 2 * virtuals * virtuals * (depth + 2 * width)
    gamma = pl.pallas_call(
        gathered_kernel,
        out_shape=jax.ShapeDtypeStruct((count, width, virtuals), jnp.bfloat16),
        in_specs=[
            pl.BlockSpec(memory_space=pl.ANY),
            pl.BlockSpec(memory_space=pltpu.SMEM),
            pl.BlockSpec(memory_space=pltpu.VMEM),
        ],
        out_specs=pl.BlockSpec(memory_space=pltpu.VMEM),
        scratch_shapes=[
            pltpu.VMEM((count, virtuals, depth), jnp.bfloat16),
            pltpu.VMEM((count, width, virtuals), jnp.bfloat16),
            pltpu.VMEM((count, width, virtuals), jnp.float32),
            pltpu.VMEM((window, ROWS), jnp.float32),
            pltpu.VMEM((virtuals, ROWS), jnp.float32),
            pltpu.SemaphoreType.DMA,
            pltpu.SemaphoreType.DMA((2, chunks)),
            pltpu.SemaphoreType.DMA((chunks,)),
            pltpu.SemaphoreType.DMA((4, chunks)),
            pltpu.SemaphoreType.DMA((8, chunks)),
        ],
        compiler_params=pltpu.CompilerParams(
            collective_id=0, has_side_effects=True, vmem_limit_bytes=44 * 1024 * 1024
        ),
        cost_estimate=pl.CostEstimate(
            flops=count * OFFSETS * pair_flops, bytes_accessed=count * virtuals * depth * 2,
            transcendentals=0,
        ),
    )(factors[0], occ_energy, vir_energy[None])
    return jnp.einsum("ipa,ma->pim", gamma, coeffs, preferred_element_type=jnp.float32).astype(
        jnp.bfloat16
    )


def fits(count, virtuals, depth):
    width = depth // count
    return (
        count == 8
        and count == 2 * OFFSETS + 2
        and virtuals % ROWS == 0
        and depth % (LANES * 2) == 0
        and width % 32 == 0
    )


def either(factors, occ_energy, vir_energy, coeffs):
    if fits(lax.axis_size("occ"), factors.shape[1], factors.shape[2]):
        return gathered(factors, occ_energy, vir_energy, coeffs)
    return on_device(factors, occ_energy, vir_energy, coeffs)


def solution(mesh):
    return jax.shard_map(
        either,
        mesh=mesh,
        in_specs=(P(("frag", "occ"), None, None), P("frag"), P("frag"), P("frag", None)),
        out_specs=P("occ", "frag", None),
        check_vma=False,
    )
```
